32 devices in a mesh: fluid: 16 (over z, x, core), solid: 2 (over y).
Axes of the slice: x: 2, y: 2, z: 4, core: 2. Of those that a mesh axis runs over, the one named last changes fastest.
Arguments:
- fluid_load: float32 [2048, 3, 128], P(('fluid', 'solid')), may hold values from -6 to 6
- stiffness: float32 [2048, 3, 128], P(('fluid', 'solid')), may hold values from 0.2 to 2
- mapping: bfloat16 [2048, 128, 128], P(('fluid', 'solid')), may hold values from -0.5 to 0.5
- live_count: int32 [32], P(('fluid', 'solid')), may hold values from 40 to 64, as said below
- dest_device: int32 [2048, 1], P(('fluid', 'solid')), may hold values from 0 to 15; in each aligned block of 64 rows (0 to 63, 64 to 127, ...) at most 8 rows name the same one
- local_block: int32 [2048], P(('fluid', 'solid')), may hold values from 0 to 3
- compliance: float32 [2, 64, 3, 128], P('solid', 'fluid'), may hold values from 0.05 to 0.5
- start_disp: float32 [2, 64, 3, 128], P('solid', 'fluid'), may hold values from -40 to 40
- residual_history: float32 [50, 2, 64, 3, 128], P(None, 'solid', 'fluid'), may hold values from -40 to 40
- update_history: float32 [50, 2, 64, 3, 128], P(None, 'solid', 'fluid'), may hold values from -2.4 to 2.4
Outputs:
- displacement: float32 [2, 64, 3, 128], P('solid', 'fluid')
- fluid_displacement: float32 [2048, 3, 128], P(('fluid', 'solid'))
The draws below stay inside these ranges and needn't reach their ends.
Inputs may be any that keep to these rules, and one draw needn't show every extreme that they name: `live_count`: each device's live blocks are its first ones; some device has exactly 64. `dest_device`: among the 64 rows of one device no fluid index appears more than 8 times.
All inputs are finite; a program needn't handle non-finite values.
Results may differ from the reference program's by a relative error of at most 0.0094.
Values may be sent and summed in bfloat16 or wider, within the bound.
A program may use at most 64 MiB of HBM per device.

```python
import math
import jax
import jax.numpy as jnp
import numpy as np
from jax import lax

FB = 64
SB_DEV = 4
BF = 128
BS = 128
HIST = 50
ITERS = 2
OWN_BLK = 64
FBLK = 2048
CAP = 8
N_FLUID = 16
N_SOLID = 2


def history_pair(key):
    n_blocks = N_SOLID * OWN_BLK
    n_total = n_blocks * 3 * BS
    subkeys = jax.random.split(key, 5)
    base_draw = jax.random.normal(subkeys[0], (HIST, n_total), jnp.float32)
    shared_part = jax.random.normal(subkeys[1], (n_total,), jnp.float32)
    mixing = jnp.eye(HIST, dtype=jnp.float32) + 0.2 * jax.random.normal(subkeys[2], (HIST, HIST), jnp.float32)
    rising = 1.0 + 2.0 * jnp.arange(n_blocks, dtype=jnp.float32) / max(n_blocks - 1, 1)
    rising = jnp.repeat(rising, 3 * BS)
    basis_draw = (jnp.dot(mixing, base_draw, precision=lax.Precision.HIGHEST) + 0.5 * shared_part[None, :]) * rising[None, :]
    coef_draw = 0.15 * jax.random.normal(subkeys[3], (HIST,), jnp.float32)
    start_draw = -jnp.dot(coef_draw, basis_draw, precision=lax.Precision.HIGHEST) + 0.3 * jax.random.normal(subkeys[4], (n_total,), jnp.float32)
    basis_draw = jnp.clip(basis_draw, -40.0, 40.0).reshape(HIST, N_SOLID, OWN_BLK, 3, BS)
    start_draw = jnp.clip(start_draw, -40.0, 40.0).reshape(N_SOLID, OWN_BLK, 3, BS)
    return (basis_draw, start_draw)


def draw_residual_history(key, part):
    return history_pair(jax.random.fold_in(key, 11))[0]


def draw_start_disp(key, part):
    return history_pair(jax.random.fold_in(key, 11))[1]


def draw_live_count(key, part):
    devices_all = N_FLUID * N_SOLID
    subkeys = jax.random.split(key, 2)
    lowest = FB * 5 // 8
    first_draw = jax.random.randint(subkeys[0], (devices_all,), lowest, FB + 1)
    chosen = jax.random.randint(subkeys[1], (), 0, devices_all)
    return jnp.where(jnp.arange(devices_all) == chosen, FB, first_draw).astype(jnp.int32)


def with_ends(values, own_key, smallest, high):
    spot = [jax.random.randint(jax.random.fold_in(own_key, axis), (), 0, length) for axis, length in enumerate(values.shape)]
    widest = values.shape.index(max(values.shape))
    next_to = spot[:widest] + [(spot[widest] + 1) % values.shape[widest]] + spot[widest + 1:]
    return values.at[tuple(spot)].set(smallest).at[tuple(next_to)].set(high)


def block_levels(rng, extent, pieces, smallest, top_value):
    def one(dim, blocks):
        draws = jax.random.uniform(jax.random.fold_in(jax.random.fold_in(rng, 6), dim), (blocks,), jnp.float32, smallest / len(pieces), top_value / len(pieces))
        return jnp.repeat(jnp.exp(draws), extent[dim] // blocks).reshape((-1,) + (1,) * (len(extent) - dim - 1))

    gain = one(*pieces[0])
    for cut in pieces[1:]:
        gain = gain * one(*cut)
    return gain


def assign_block(rng, own, number, rows, amount, top, reach, lean):
    sequence = jax.random.permutation(rng, amount)
    crowded, ordinary = shares(amount, rows * top, reach, lean, True), shares(amount, rows * top, reach, lean, False)
    places = jnp.arange(amount)

    def named(lengths, turn):
        used = int((lengths > 0).sum())
        fixed = max(1, used // 4)
        moved = fixed + (places - fixed + turn * (used - fixed)) % max(1, amount - fixed)
        return jnp.zeros((amount,), jnp.int32).at[sequence[jnp.where(places < fixed, places, moved)]].set(jnp.asarray(lengths, jnp.int32))

    lengths = jnp.where(number % 4 == 0, named(crowded, number // 4), named(ordinary, number - number // 4 - 1))
    mixed = jax.random.permutation(jax.random.fold_in(own, 3), amount)
    source_of, receiver = mixed[0:amount // 2 * 2:2], mixed[1:amount // 2 * 2:2]
    margin = jnp.minimum(lengths[source_of] - 1, reach - lengths[receiver]) // 2
    margin = jnp.where((source_of == sequence[0]) | (receiver == sequence[0]) | (lengths[receiver] == 0), 0, jnp.maximum(margin, 0))
    moved = jax.random.randint(jax.random.fold_in(own, 4), (amount // 2,), 0, 1 << 20) % (margin + 1)
    lengths = lengths.at[source_of].add(-moved).at[receiver].add(moved)
    items = jnp.searchsorted(jnp.cumsum(lengths), jnp.arange(rows * top), side="right").astype(jnp.int32)
    table = items.reshape(top, rows).T
    table = table[jax.random.permutation(jax.random.fold_in(own, 1), rows)]
    turn = jax.random.randint(jax.random.fold_in(own, 2), (rows, 1), 0, top)
    return jnp.take_along_axis(table, (jnp.arange(top)[None, :] + turn) % top, axis=1)


def shares(amount, total, reach, slope, full):
    portions = [(1 << 20) // math.isqrt(rank ** slope) + 1 for rank in range(1, amount + 1)]
    largest = reach if full else min(reach, max(-(-total // amount), total * portions[0] // sum(portions)))
    least = 1 if total - largest >= amount - 1 else 0
    given, surplus = [largest] + [least] * (amount - 1), total - largest - least * (amount - 1)
    while surplus > 0:
        free = [i for i in range(1, amount) if given[i] < largest] or [i for i in range(1, amount) if given[i] < reach]
        whole, remaining = sum([portions[i] for i in free]), surplus
        for i in free:
            addition = min(reach - given[i], max(1, remaining * portions[i] // whole), surplus)
            given[i] = given[i] + addition
            surplus = surplus - addition
    return np.array(given)


def centred(rng, extent, spread, bound, pieces=(), kind=jnp.bfloat16):
    level = block_levels(rng, extent, pieces, -0.22, 0.18) if pieces else 1.0
    result = jax.random.normal(rng, extent, jnp.float32) * spread * level
    return jnp.minimum(jnp.maximum(result, -bound), bound).astype(kind)


def setup_inputs(seed: int = 0) -> dict:
    keys = jax.random.split(jax.random.key(seed), 11)
    fluid_load = centred(keys[0], (FBLK, 3, BF), 1.0, 6.0, ((0, 32),), jnp.float32)
    stiffness = jnp.clip(jnp.exp(math.log(2.0) - 2.3025851 * jax.random.uniform(keys[1], (FBLK, 3, BF), jnp.float32) ** block_levels(keys[1], (FBLK, 3, BF), ((0, 32),), -0.2, 0.2)), 0.2, 2.0)
    mapping = centred(keys[2], (FBLK, BS, BF), BF ** -0.5, 0.5, ((0, 32),))
    live_count = draw_live_count(jax.random.fold_in(keys[10], 71), 0)
    dest_device_keys = jax.random.split(jax.random.fold_in(keys[4], 1), FBLK // FB)
    dest_device_turns = jax.random.permutation(jax.random.fold_in(keys[4], 3), FBLK // FB)
    dest_device = jax.vmap(lambda own, number: assign_block(jax.random.fold_in(keys[4], 2), own, number, FB, N_FLUID, 1, CAP, 0))(dest_device_keys, dest_device_turns).reshape((FBLK, 1))
    local_block = with_ends(jax.random.randint(keys[5], (FBLK,), 0, SB_DEV), jax.random.fold_in(keys[5], 1), 0, SB_DEV - 1).astype(jnp.int32)
    compliance = jnp.clip(jnp.exp(math.log(0.5) - 2.3025851 * jax.random.uniform(keys[6], (N_SOLID, OWN_BLK, 3, BS), jnp.float32) ** block_levels(keys[6], (N_SOLID, OWN_BLK, 3, BS), ((0, 2), (1, 16)), -0.2, 0.2)), 0.05, 0.5)
    start_disp = draw_start_disp(jax.random.fold_in(keys[10], 71), 0)
    residual_history = draw_residual_history(jax.random.fold_in(keys[10], 71), 0)
    update_history = centred(keys[9], (HIST, N_SOLID, OWN_BLK, 3, BS), 0.3, 2.4, ((1, 2), (2, 16)), jnp.float32)
    return dict(fluid_load=fluid_load, stiffness=stiffness, mapping=mapping, live_count=live_count, dest_device=dest_device, local_block=local_block, compliance=compliance, start_disp=start_disp, residual_history=residual_history, update_history=update_history)


ridge_share = 0.01

def solve_small(gram_matrix, right_side):
    order = gram_matrix.shape[0]
    ridge = ridge_share * jnp.trace(gram_matrix) / order
    factor = jnp.linalg.cholesky(gram_matrix + ridge * jnp.eye(order, dtype=gram_matrix.dtype))
    halfway = lax.linalg.triangular_solve(factor, right_side[:, None], left_side=True, lower=True)
    solved = lax.linalg.triangular_solve(factor, halfway, left_side=True, lower=True, transpose_a=True)
    return -solved[:, 0]

def reference(fluid_load, stiffness, mapping, live_count, dest_device, local_block, compliance, start_disp, residual_history, update_history):
    devices_all = N_FLUID * N_SOLID
    block_ids = jnp.arange(FBLK, dtype=jnp.int32)
    device_of = block_ids // FB
    alive = (block_ids % FB < live_count[device_of]).astype(jnp.float32)[:, None, None]
    target = (device_of % N_SOLID * OWN_BLK + dest_device[:, 0] * SB_DEV + local_block).astype(jnp.int32)
    mapping_dev = mapping.reshape(devices_all, FB, BS, BF)
    target_dev = target.reshape(devices_all, FB)

    def to_fluid(struct_disp):
        packed = struct_disp.astype(jnp.bfloat16).reshape(N_SOLID * OWN_BLK, 3, BS)

        def apply_back(scan_item):
            block_map, block_target = scan_item
            picked = packed[block_target]
            return jnp.einsum('bjn,bcj->bcn', block_map.astype(jnp.float32), picked.astype(jnp.float32))
        fluid_disp = lax.map(apply_back, (mapping_dev, target_dev)).reshape(FBLK, 3, BF)
        return fluid_disp * alive

    def to_solid(fluid_disp):
        fluid_force = (alive * (fluid_load - stiffness * fluid_disp)).astype(jnp.bfloat16)
        fluid_force = fluid_force.reshape(devices_all, FB, 3, BF)

        def accumulate(summed, scan_item):
            block_map, block_force, block_target = scan_item
            contrib = jnp.einsum('bjn,bcn->bcj', block_map.astype(jnp.float32), block_force.astype(jnp.float32))
            return (summed.at[block_target].add(contrib), None)
        summed0 = jnp.zeros((N_SOLID * OWN_BLK, 3, BS), jnp.float32)
        summed, _ = lax.scan(accumulate, summed0, (mapping_dev, fluid_force, target_dev))
        return summed.reshape(N_SOLID, OWN_BLK, 3, BS)
    struct_disp = start_disp
    basis_cols = residual_history
    updates = update_history
    last_resid = struct_disp
    last_image = struct_disp
    for iteration in range(ITERS):
        fluid_disp = to_fluid(struct_disp)
        struct_image = compliance * to_solid(fluid_disp)
        residual = struct_image - struct_disp
        if iteration > 0:
            basis_cols = jnp.concatenate([basis_cols[1:], (residual - last_resid)[None]], 0)
            updates = jnp.concatenate([updates[1:], (struct_image - last_image)[None]], 0)
        basis_flat = basis_cols.reshape(HIST, -1)
        resid_flat = residual.reshape(-1)
        gram_matrix = jnp.dot(basis_flat, basis_flat.T, precision=lax.Precision.HIGHEST)
        right_side = jnp.dot(basis_flat, resid_flat, precision=lax.Precision.HIGHEST)
        coefficients = solve_small(gram_matrix, right_side)
        struct_disp = struct_image + jnp.tensordot(coefficients, updates, axes=1, precision=lax.Precision.HIGHEST)
        last_resid = residual
        last_image = struct_image
    final_disp = to_fluid(struct_disp)
    return (struct_disp, final_disp)
```

```python
import functools

import jax
import jax.numpy as jnp
from jax import lax
from jax.experimental import pallas as pl
from jax.experimental.pallas import tpu as pltpu
from jax.sharding import PartitionSpec as P

ridge_share = 0.01
MESH = pl.DeviceIdType.MESH
HIGH = lax.Precision.HIGHEST
F32 = jnp.float32
BF16 = jnp.bfloat16
NT = (((1,), (1,)), ((), ()))
HALF = 64
FORCE_TYPE = F32


def eliminate(m, order):
    rows = lax.broadcasted_iota(jnp.int32, m.shape, 0)
    for k in range(order):
        col = jnp.broadcast_to(m[:, k : k + 1], m.shape)
        row = m[k : k + 1, :] / col[k : k + 1, :]
        m = jnp.where(rows == k, row, m - col * row)
    return m


def kernel(
    nf, ns, dims,
    load_hbm, stiff_hbm, map_hbm, live, dest, local, comp, start, hist_hbm, upd_hbm,
    disp, fluid_out,
    mapping, loads, stiffs, hist, upd, comp16, x16,
    onehot, onehot_t, picked, contrib, u_out,
    xg, fs, fr, bg, gs, gr, gf,
    in_sems, out_sems, x_send, x_recv, f_send, f_recv, b_send, b_recv, g_send, g_recv,
):
    blocks, sub, order, iters = dims
    nd = nf * ns
    groups = blocks // 8
    slot = 4 * sub
    owners = HALF // 8
    fi = lax.axis_index("fluid")
    si = lax.axis_index("solid")
    me = fi * ns + si

    copies = [pltpu.make_async_copy(map_hbm, mapping, in_sems.at[0])]
    for c in range(3):
        copies.append(pltpu.make_async_copy(load_hbm.at[:, c], loads.at[c], in_sems.at[1 + c]))
        copies.append(pltpu.make_async_copy(stiff_hbm.at[:, c], stiffs.at[c], in_sems.at[4 + c]))
    hist_copies = []
    upd_copies = []
    for t in range(sub):
        for c in range(3):
            k = 3 * t + c
            hist_copies.append(
                pltpu.make_async_copy(
                    hist_hbm.at[:, 0, t, c], hist.at[k, pl.ds(0, order)], in_sems.at[7 + k]
                )
            )
            upd_copies.append(
                pltpu.make_async_copy(
                    upd_hbm.at[:, 0, t, c], upd.at[k, pl.ds(0, order)], in_sems.at[7 + 3 * sub + k]
                )
            )
    for copy in hist_copies + copies + upd_copies:
        copy.start()

    barrier = pltpu.get_barrier_semaphore()

    def greet(o, carry):
        p = lax.rem(me + o, nd)
        pl.semaphore_signal(barrier, inc=1, device_id=(p // ns, lax.rem(p, ns)), device_id_type=MESH)
        return carry

    lax.fori_loop(1, nd, greet, 0)

    comp16[...] = jnp.zeros_like(comp16)
    x16[...] = jnp.zeros_like(x16)
    for t in range(sub):
        comp16[4 * t : 4 * t + 3] = comp[0, t]
        x16[4 * t : 4 * t + 3] = start[0, t]
    for k in range(3 * sub):
        hist[k, order:] = jnp.zeros((HALF - order, 128), F32)
        upd[k, order:] = jnp.zeros((HALF - order, 128), F32)

    x = x16[...]
    xg[0, fi] = x.astype(BF16)

    eye = lax.broadcasted_iota(jnp.int32, (blocks, blocks), 0) == lax.broadcasted_iota(
        jnp.int32, (blocks, blocks), 1
    )
    local_col = jnp.sum(
        jnp.where(eye, jnp.broadcast_to(local[...].astype(F32), (blocks, blocks)), 0.0), axis=1, keepdims=True
    )
    row_id = lax.broadcasted_iota(jnp.int32, (blocks, 1), 0)
    first = dest[...].astype(F32) * slot + local_col * 4.0
    first = jnp.where(row_id < live[0], first, -8.0)
    parts = []
    for g in range(groups):
        one = first[8 * g : 8 * g + 8]
        parts += [one, one + 1.0, one + 2.0, jnp.full((8, 1), -8.0, F32)]
    target = jnp.concatenate(parts, axis=0)
    n_rows = 4 * blocks
    n_slots = nf * slot
    slot_id = lax.broadcasted_iota(jnp.int32, (n_rows, n_slots), 1).astype(F32)
    onehot[...] = jnp.where(slot_id == target, 1.0, 0.0).astype(BF16)
    diag = lax.broadcasted_iota(jnp.int32, (n_rows, n_rows), 0) == lax.broadcasted_iota(
        jnp.int32, (n_rows, n_rows), 1
    )
    target_row = jnp.sum(jnp.where(diag, jnp.broadcast_to(target, (n_rows, n_rows)), 0.0), axis=0, keepdims=True)
    slot_col = lax.broadcasted_iota(jnp.int32, (n_slots, n_rows), 0).astype(F32)
    onehot_t[...] = jnp.where(slot_col == target_row, 1.0, 0.0).astype(BF16)

    pl.semaphore_wait(barrier, nd - 1)

    def send_x(phase):
        def step(o, carry):
            p = lax.rem(fi + o, nf)
            pltpu.make_async_remote_copy(
                src_ref=xg.at[phase, fi], dst_ref=xg.at[phase, fi],
                send_sem=x_send.at[phase], recv_sem=x_recv.at[phase],
                device_id=(p, si), device_id_type=MESH,
            ).start()
            return carry

        lax.fori_loop(1, nf, step, 0)

    def wait_bytes(ref, sem):
        pltpu.make_async_copy(ref, ref, sem).wait()

    def send_f(phase):
        def step(o, carry):
            p = lax.rem(fi + o, nf)
            pltpu.make_async_remote_copy(
                src_ref=fs.at[phase, p], dst_ref=fr.at[phase, fi],
                send_sem=f_send.at[phase], recv_sem=f_recv.at[phase],
                device_id=(p, si), device_id_type=MESH,
            ).start()
            return carry

        lax.fori_loop(1, nf, step, 0)

    def send_all(ref, send_sem, recv_sem):
        def step(o, carry):
            p = lax.rem(me + o, nd)
            pltpu.make_async_remote_copy(
                src_ref=ref, dst_ref=ref, send_sem=send_sem, recv_sem=recv_sem,
                device_id=(p // ns, lax.rem(p, ns)), device_id_type=MESH,
            ).start()
            return carry

        lax.fori_loop(1, nd, step, 0)

    send_x(0)

    for copy in hist_copies:
        copy.wait()
    gram = jnp.zeros((HALF, HALF), F32)
    for k in range(3 * sub):
        v = hist[k]
        gram = gram + lax.dot_general(v, v, NT, precision=HIGH, preferred_element_type=F32)
    gram = jnp.concatenate([gram, jnp.zeros((HALF, 128 - HALF), F32)], axis=1)
    for o in range(owners):
        gs[o] = gram[8 * o : 8 * o + 8]
    for o in range(owners):
        @pl.when(me == o)
        def _():
            gr[me] = gs[o]

        @pl.when(me != o)
        def _():
            pltpu.make_async_remote_copy(
                src_ref=gs.at[o], dst_ref=gr.at[me], send_sem=g_send.at[0], recv_sem=g_recv.at[0],
                device_id=(o // ns, o % ns), device_id_type=MESH,
            ).start()

    mod8 = lax.rem(lax.broadcasted_iota(jnp.int32, (32, 128), 0), 8)

    def pick(phase):
        wait_bytes(xg.at[phase, pl.ds(0, nf - 1)], x_recv.at[phase])
        x_all = xg[phase].reshape(n_slots, 128)
        picked[...] = jnp.dot(onehot[...], x_all, preferred_element_type=F32)

    def to_fluid(g):
        rows = picked[32 * g : 32 * g + 32]
        lhs = jnp.concatenate([jnp.where(mod8 == i, rows, 0.0).astype(BF16) for i in range(8)], axis=1)
        return jnp.dot(lhs, mapping[8 * g : 8 * g + 8].reshape(8 * 128, 128), preferred_element_type=F32)

    def to_solid(g, u):
        force = []
        for c in range(3):
            span = slice(8 * g, 8 * g + 8)
            force.append(loads[c, span] - stiffs[c, span] * u[8 * c : 8 * c + 8])
        force = jnp.concatenate(force + [jnp.zeros((8, 128), F32)], axis=0)
        total = jnp.zeros((32, 128), F32)
        for i in range(8):
            total = total + lax.dot_general(
                jnp.where(mod8 == i, force, 0.0).astype(BF16), mapping[8 * g + i], NT, preferred_element_type=F32
            )
        return total

    resid = image = None
    inverse = gram_all = None
    lanes = lax.broadcasted_iota(jnp.int32, (HALF, 128), 1)
    rows = lax.broadcasted_iota(jnp.int32, (HALF, 128), 0)
    for it in range(iters):
        pick(it)
        if it == 0:
            for copy in copies:
                copy.wait()
        for g in range(groups):
            contrib[32 * g : 32 * g + 32] = to_solid(g, to_fluid(g))
        part = contrib[...]
        high = part.astype(BF16)
        low = (part - high.astype(F32)).astype(BF16)
        total = jnp.dot(onehot_t[...], high, preferred_element_type=F32) + jnp.dot(
            onehot_t[...], low, preferred_element_type=F32
        )
        fs[it] = total.reshape(nf, slot, 128).astype(FORCE_TYPE)
        fr[it, fi] = fs[it, fi]
        send_f(it)

        if it == 0:
            @pl.when(me < owners)
            def _():
                wait_bytes(gr.at[pl.ds(0, nd - 1)], g_recv.at[0])
                gf[me] = jnp.sum(gr[...], axis=0)
                send_all(gf.at[me], g_send.at[1], g_recv.at[1])

        wait_bytes(fr.at[it, pl.ds(0, nf - 1)], f_recv.at[it])
        new_image = comp16[...] * jnp.sum(fr[it].astype(F32), axis=0)
        new_resid = new_image - x
        acc_r = jnp.zeros((HALF, 128), F32)
        acc_d = jnp.zeros((HALF, 128), F32)
        if it == 0:
            for k in range(3 * sub):
                at = 4 * (k // 3) + k % 3
                acc_r = acc_r + hist[k] * new_resid[at : at + 1]
        else:
            newest = new_resid - resid
            shift = new_image - image
            for k in range(3 * sub):
                at = 4 * (k // 3) + k % 3
                hist[k, order : order + 1] = newest[at : at + 1]
                upd[k, order : order + 1] = shift[at : at + 1]
            for k in range(3 * sub):
                at = 4 * (k // 3) + k % 3
                acc_r = acc_r + hist[k] * new_resid[at : at + 1]
                acc_d = acc_d + hist[k] * newest[at : at + 1]
        resid, image = new_resid, new_image
        acc = jnp.concatenate([acc_d, acc_r], axis=0)
        sums = lax.dot_general(jnp.ones((8, 128), F32), acc, NT, precision=HIGH, preferred_element_type=F32)
        bg[it, me] = sums[0:1]
        send_all(bg.at[it, me], b_send.at[it], b_recv.at[it])

        if it == 0:
            @pl.when(me < owners)
            def _():
                wait_bytes(gf.at[pl.ds(0, owners - 1)], g_recv.at[1])

            @pl.when(me >= owners)
            def _():
                wait_bytes(gf, g_recv.at[1])

            gram_all = gf[...].reshape(HALF, 128)
            trace = jnp.sum(jnp.where(lanes == rows, gram_all, 0.0), keepdims=True)
            ridge = ridge_share * trace / order
            inside = (rows < order)
            matrix = gram_all + jnp.where(lanes == rows, jnp.where(inside, ridge, 1.0), 0.0)
            matrix = matrix + jnp.where(lanes == rows + HALF, 1.0, 0.0)
            inverse = eliminate(matrix, order)
            for copy in upd_copies:
                copy.wait()

        wait_bytes(bg.at[it, pl.ds(0, nd - 1)], b_recv.at[it])
        sums = jnp.sum(bg[it], axis=0)
        if it == 0:
            coef = -jnp.sum(jnp.where(lanes >= HALF, inverse * sums, 0.0), axis=1, keepdims=True)
        else:
            column = jnp.sum(jnp.where(lanes == rows, sums, 0.0), axis=1, keepdims=True)
            right = jnp.sum(jnp.where(lanes == rows + HALF, sums, 0.0), axis=1, keepdims=True)
            old = (rows >= 1) & (rows < order) & (lanes >= 1) & (lanes < order)
            matrix = jnp.where(old, gram_all, 0.0)
            matrix = jnp.where((rows == order) & (lanes >= 1) & (lanes <= order), sums, matrix)
            matrix = jnp.where((lanes == order) & (rows >= 1) & (rows < order), column, matrix)
            trace = jnp.sum(jnp.where(lanes == rows, matrix, 0.0), keepdims=True)
            ridge = ridge_share * trace / order
            inside = (rows >= 1) & (rows <= order)
            matrix = matrix + jnp.where(lanes == rows, jnp.where(inside, ridge, 1.0), 0.0)
            matrix = jnp.where(lanes == HALF, jnp.where(inside, right, 0.0), matrix)
            solved = eliminate(matrix, order + 1)
            coef = -solved[:, HALF : HALF + 1]
        pieces = []
        for t in range(sub):
            for c in range(3):
                pieces.append(jnp.sum(upd[3 * t + c] * coef, axis=0, keepdims=True))
            pieces.append(jnp.zeros((1, 128), F32))
        x = image + jnp.concatenate(pieces, axis=0)
        xg[it + 1, fi] = x.astype(BF16)
        send_x(it + 1)

    for t in range(sub):
        disp[0, t] = x[4 * t : 4 * t + 3]

    pick(iters)
    for g in range(groups):
        u = to_fluid(g)
        for c in range(3):
            u_out[c, 8 * g : 8 * g + 8] = u[8 * c : 8 * c + 8]
    out_copies = [
        pltpu.make_async_copy(u_out.at[c], fluid_out.at[:, c], out_sems.at[c]) for c in range(3)
    ]
    for copy in out_copies:
        copy.start()

    for phase in range(iters + 1):
        wait_bytes(xg.at[phase, pl.ds(0, nf - 1)], x_send.at[phase])
    for phase in range(iters):
        wait_bytes(fr.at[phase, pl.ds(0, nf - 1)], f_send.at[phase])
        wait_bytes(bg.at[phase, pl.ds(0, nd - 1)], b_send.at[phase])
    @pl.when(me >= owners)
    def _():
        wait_bytes(gs, g_send.at[0])

    @pl.when(me < owners)
    def _():
        wait_bytes(gs.at[pl.ds(0, owners - 1)], g_send.at[0])
        wait_bytes(gr.at[pl.ds(0, nd - 1)], g_send.at[1])

    for copy in out_copies:
        copy.wait()


def body(load, stiff, mapping, live, dest, local, comp, start, hist, upd, *, nf, ns):
    blocks = mapping.shape[0]
    sub = comp.shape[1]
    order = hist.shape[0]
    iters = 2
    nd = nf * ns
    slot = 4 * sub
    owners = HALF // 8
    vmem = pl.BlockSpec(memory_space=pltpu.VMEM)
    smem = pl.BlockSpec(memory_space=pltpu.SMEM)
    hbm = pl.BlockSpec(memory_space=pl.ANY)
    dma = pltpu.SemaphoreType.DMA
    return pl.pallas_call(
        functools.partial(kernel, nf, ns, (blocks, sub, order, iters)),
        out_shape=(
            jax.ShapeDtypeStruct(comp.shape, F32),
            jax.ShapeDtypeStruct(load.shape, F32),
        ),
        in_specs=[hbm, hbm, hbm, smem, vmem, vmem, vmem, vmem, hbm, hbm],
        out_specs=(vmem, hbm),
        scratch_shapes=[
            pltpu.VMEM(mapping.shape, BF16),
            pltpu.VMEM((3, blocks, 128), F32),
            pltpu.VMEM((3, blocks, 128), F32),
            pltpu.VMEM((3 * sub, HALF, 128), F32),
            pltpu.VMEM((3 * sub, HALF, 128), F32),
            pltpu.VMEM((slot, 128), F32),
            pltpu.VMEM((slot, 128), F32),
            pltpu.VMEM((4 * blocks, nf * slot), BF16),
            pltpu.VMEM((nf * slot, 4 * blocks), BF16),
            pltpu.VMEM((4 * blocks, 128), F32),
            pltpu.VMEM((4 * blocks, 128), F32),
            pltpu.VMEM((3, blocks, 128), F32),
            pltpu.VMEM((iters + 1, nf, slot, 128), BF16),
            pltpu.VMEM((iters, nf, slot, 128), FORCE_TYPE),
            pltpu.VMEM((iters, nf, slot, 128), FORCE_TYPE),
            pltpu.VMEM((iters, nd, 1, 128), F32),
            pltpu.VMEM((owners, 8, 128), F32),
            pltpu.VMEM((nd, 8, 128), F32),
            pltpu.VMEM((owners, 8, 128), F32),
            dma((7 + 6 * sub,)),
            dma((3,)),
            dma((iters + 1,)),
            dma((iters + 1,)),
            dma((iters,)),
            dma((iters,)),
            dma((iters,)),
            dma((iters,)),
            dma((2,)),
            dma((2,)),
        ],
        compiler_params=pltpu.CompilerParams(collective_id=0, has_side_effects=True),
    )(load, stiff, mapping, live, dest, local.reshape(1, blocks), comp, start, hist, upd)


def solution(mesh):
    in_specs = (
        P(("fluid", "solid"), None, None),
        P(("fluid", "solid"), None, None),
        P(("fluid", "solid"), None, None),
        P(("fluid", "solid")),
        P(("fluid", "solid"), None),
        P(("fluid", "solid")),
        P("solid", "fluid", None, None),
        P("solid", "fluid", None, None),
        P(None, "solid", "fluid", None, None),
        P(None, "solid", "fluid", None, None),
    )
    out_specs = (P("solid", "fluid", None, None), P(("fluid", "solid"), None, None))
    inner = functools.partial(body, nf=mesh.shape["fluid"], ns=mesh.shape["solid"])
    return jax.shard_map(inner, mesh=mesh, in_specs=in_specs, out_specs=out_specs, check_vma=False)
```

```python
import functools

import jax
import jax.numpy as jnp
from jax import lax
from jax.experimental import pallas as pl
from jax.experimental.pallas import tpu as pltpu
from jax.sharding import PartitionSpec as P

ridge_share = 0.01
MESH = pl.DeviceIdType.MESH
HIGH = lax.Precision.HIGHEST
F32 = jnp.float32
BF16 = jnp.bfloat16
NT = (((1,), (1,)), ((), ()))
HALF = 64
FORCE_TYPE = BF16


def eliminate(m, first, last):
    rows = lax.broadcasted_iota(jnp.int32, m.shape, 0)
    for k in range(first, last, 2):
        a = jnp.broadcast_to(m[:, k : k + 1], m.shape)
        b = jnp.broadcast_to(m[:, k + 1 : k + 2], m.shape)
        p, q = a[k : k + 1], b[k : k + 1]
        u, v = a[k + 1 : k + 2], b[k + 1 : k + 2]
        over = 1.0 / (p * v - q * u)
        top, low = m[k : k + 1], m[k + 1 : k + 2]
        new_top = (v * top - q * low) * over
        new_low = (p * low - u * top) * over
        m = m - a * new_top - b * new_low
        m = jnp.where(rows == k, new_top, jnp.where(rows == k + 1, new_low, m))
    return m


def send_order(n):
    return sorted(range(1, n), key=lambda o: -min(o, n - o))


def loop(n, step):
    if n <= 16:
        for o in send_order(n):
            step(o)
    else:
        def one(o, carry):
            step(o)
            return carry

        lax.fori_loop(1, n, one, 0)


def wrap(a, n):
    return jnp.where(a >= n, a - n, a)


def kernel(
    nf, ns, dims,
    load_hbm, stiff_hbm, map_hbm, live_hbm, dest_hbm, local_hbm, comp_hbm, start_hbm, hist_hbm, upd_hbm,
    disp, delta, fluid_out,
    live, dest, local, comp, start,
    mapping, loads, stiffs, hist, upd, comp16, x16,
    onehot, onehot_t, picked, contrib, u_out,
    xg, fs, fr, bg, gs, gr, gf,
    small_sems, in_sems, out_sems, x_send, x_recv, f_send, f_recv, b_send, b_recv, g_send, g_recv,
):
    blocks, sub, order, iters = dims
    nd = nf * ns
    groups = blocks // 8
    slot = -(-3 * sub // 16) * 16
    owners = HALF // 8
    used = 3 * sub
    tall = -(-(order + 2) // 8) * 8
    fi = lax.axis_index("fluid")
    si = lax.axis_index("solid")
    me = fi * ns + si

    def everyone(step):
        def with_all(o):
            for k in range(ns):
                step(wrap(fi + o, nf), wrap(si + k, ns))

        loop(nf, with_all)
        for k in range(1, ns):
            step(fi, wrap(si + k, ns))

    barrier = pltpu.get_barrier_semaphore()
    xg[:, :, used:] = jnp.zeros((iters + 1, nf, slot - used, 128), BF16)
    fr[:, :, used:] = jnp.zeros((iters, nf, slot - used, 128), FORCE_TYPE)

    def greet(p, q):
        pl.semaphore_signal(barrier, inc=1, device_id=(p, q), device_id_type=MESH)

    small = [
        pltpu.make_async_copy(ref, to, small_sems.at[i])
        for i, (ref, to) in enumerate(
            [(live_hbm, live), (dest_hbm, dest), (local_hbm, local), (comp_hbm, comp), (start_hbm, start)]
        )
    ]
    for copy in small:
        copy.start()
    everyone(greet)

    copies = [pltpu.make_async_copy(map_hbm, mapping, in_sems.at[0])]
    for c in range(3):
        copies.append(pltpu.make_async_copy(load_hbm.at[c], loads.at[c], in_sems.at[1 + c]))
        copies.append(pltpu.make_async_copy(stiff_hbm.at[c], stiffs.at[c], in_sems.at[4 + c]))
    hist_copies = []
    upd_copies = []
    for c in range(3):
        for t in range(sub):
            k = sub * c + t
            hist_copies.append(
                pltpu.make_async_copy(
                    hist_hbm.at[:, 0, c, t], hist.at[k, pl.ds(0, order)], in_sems.at[7 + k]
                )
            )
            upd_copies.append(
                pltpu.make_async_copy(
                    upd_hbm.at[:, 0, c, t], upd.at[k, pl.ds(0, order)], in_sems.at[7 + 3 * sub + k]
                )
            )
    for copy in hist_copies + copies + upd_copies:
        copy.start()

    for copy in small:
        copy.wait()
    comp16[...] = jnp.zeros_like(comp16)
    x16[...] = jnp.zeros_like(x16)
    for c in range(3):
        comp16[sub * c : sub * c + sub] = comp[0, c]
        x16[sub * c : sub * c + sub] = start[0, c]
    for k in range(3 * sub):
        hist[k, order:] = jnp.zeros((HALF - order, 128), F32)
        upd[k, order:] = jnp.zeros((HALF - order, 128), F32)

    x = x16[...]
    xg[0, fi, :used] = x[:used].astype(BF16)

    eye = lax.broadcasted_iota(jnp.int32, (blocks, blocks), 0) == lax.broadcasted_iota(
        jnp.int32, (blocks, blocks), 1
    )
    base = dest[...].astype(F32) * slot + local[...].astype(F32)
    column_id = lax.broadcasted_iota(jnp.int32, (1, blocks), 1)
    base = jnp.where(column_id < live[...], base, -3.0 * slot)
    first = jnp.sum(jnp.where(eye, jnp.broadcast_to(base, (blocks, blocks)), 0.0), axis=1, keepdims=True)
    parts = []
    for g in range(groups):
        one = first[8 * g : 8 * g + 8]
        parts += [one, one + sub, one + 2.0 * sub, jnp.full((8, 1), -1.0, F32)]
    target = jnp.concatenate(parts, axis=0)
    n_rows = 4 * blocks
    n_slots = nf * slot
    slot_id = lax.broadcasted_iota(jnp.int32, (n_rows, n_slots), 1).astype(F32)
    onehot[...] = jnp.where(slot_id == target, 1.0, 0.0).astype(BF16)
    diag = lax.broadcasted_iota(jnp.int32, (n_rows, n_rows), 0) == lax.broadcasted_iota(
        jnp.int32, (n_rows, n_rows), 1
    )
    target_row = jnp.sum(jnp.where(diag, jnp.broadcast_to(target, (n_rows, n_rows)), 0.0), axis=0, keepdims=True)
    slot_col = lax.broadcasted_iota(jnp.int32, (n_slots, n_rows), 0).astype(F32)
    onehot_t[...] = jnp.where(slot_col == target_row, 1.0, 0.0).astype(BF16)

    with jax.named_scope("wait_barrier"):
        pl.semaphore_wait(barrier, nd - 1)

    def send_x(phase):
        def step(o):
            p = wrap(fi + o, nf)
            pltpu.make_async_remote_copy(
                src_ref=xg.at[phase, fi, pl.ds(0, used)], dst_ref=xg.at[phase, fi, pl.ds(0, used)],
                send_sem=x_send.at[phase], recv_sem=x_recv.at[phase],
                device_id=(p, si), device_id_type=MESH,
            ).start()

        loop(nf, step)

    def wait_bytes(ref, sem):
        pltpu.make_async_copy(ref, ref, sem).wait()

    def send_f(phase):
        def step(o):
            p = wrap(fi + o, nf)
            pltpu.make_async_remote_copy(
                src_ref=fs.at[phase, p, pl.ds(0, used)], dst_ref=fr.at[phase, fi, pl.ds(0, used)],
                send_sem=f_send.at[phase], recv_sem=f_recv.at[phase],
                device_id=(p, si), device_id_type=MESH,
            ).start()

        loop(nf, step)

    def send_all(ref, send_sem, recv_sem):
        def step(p, q):
            pltpu.make_async_remote_copy(
                src_ref=ref, dst_ref=ref, send_sem=send_sem, recv_sem=recv_sem,
                device_id=(p, q), device_id_type=MESH,
            ).start()

        everyone(step)

    send_x(0)

    for copy in hist_copies:
        copy.wait()
    gram = jnp.zeros((HALF, HALF), F32)
    for k in range(3 * sub):
        v = hist[k]
        gram = gram + lax.dot_general(v, v, NT, precision=HIGH, preferred_element_type=F32)
    gram = jnp.concatenate([gram, jnp.zeros((HALF, 128 - HALF), F32)], axis=1)
    for o in range(owners):
        gs[o] = gram[8 * o : 8 * o + 8]
    for o in range(owners):
        @pl.when(me == o)
        def _():
            gr[me] = gs[o]

        @pl.when(me != o)
        def _():
            pltpu.make_async_remote_copy(
                src_ref=gs.at[o], dst_ref=gr.at[me], send_sem=g_send.at[0], recv_sem=g_recv.at[0],
                device_id=(o // ns, o % ns), device_id_type=MESH,
            ).start()

    mod8 = lax.rem(lax.broadcasted_iota(jnp.int32, (32, 128), 0), 8)

    def pick(phase):
        with jax.named_scope("wait_x"):
            wait_bytes(xg.at[phase, pl.ds(0, nf - 1), pl.ds(0, used)], x_recv.at[phase])
        x_all = xg[phase].reshape(n_slots, 128)
        picked[...] = jnp.dot(onehot[...], x_all, preferred_element_type=F32)

    def to_fluid(g):
        rows = picked[32 * g : 32 * g + 32]
        lhs = jnp.concatenate([jnp.where(mod8 == i, rows, 0.0).astype(BF16) for i in range(8)], axis=1)
        return jnp.dot(lhs, mapping[8 * g : 8 * g + 8].reshape(8 * 128, 128), preferred_element_type=F32)

    def to_solid(g, u):
        force = []
        for c in range(3):
            span = slice(8 * g, 8 * g + 8)
            force.append(loads[c, span] - stiffs[c, span] * u[8 * c : 8 * c + 8])
        force = jnp.concatenate(force + [jnp.zeros((8, 128), F32)], axis=0)
        total = jnp.zeros((32, 128), F32)
        for i in range(8):
            total = total + lax.dot_general(
                jnp.where(mod8 == i, force, 0.0).astype(BF16), mapping[8 * g + i], NT, preferred_element_type=F32
            )
        return total

    resid = image = None
    inverse = gram_all = None
    lanes = lax.broadcasted_iota(jnp.int32, (HALF, 128), 1)
    rows = lax.broadcasted_iota(jnp.int32, (HALF, 128), 0)
    for it in range(iters):
        pick(it)
        if it == 0:
            with jax.named_scope("wait_in"):
                for copy in copies:
                    copy.wait()
        with jax.named_scope("blocks"):
            for g in range(groups):
                contrib[32 * g : 32 * g + 32] = to_solid(g, to_fluid(g))
        part = contrib[...]
        high = part.astype(BF16)
        low = (part - high.astype(F32)).astype(BF16)
        total = jnp.dot(onehot_t[...], high, preferred_element_type=F32) + jnp.dot(
            onehot_t[...], low, preferred_element_type=F32
        )
        fs[it] = total.reshape(nf, slot, 128).astype(FORCE_TYPE)
        fr[it, fi, :used] = fs[it, fi, :used]
        send_f(it)

        if it == 0:
            @pl.when(me < owners)
            def _():
                wait_bytes(gr.at[pl.ds(0, nd - 1)], g_recv.at[0])
                gf[me] = jnp.sum(gr[...], axis=0)
                send_all(gf.at[me], g_send.at[1], g_recv.at[1])

        with jax.named_scope("wait_f"):
            wait_bytes(fr.at[it, pl.ds(0, nf - 1), pl.ds(0, used)], f_recv.at[it])
        new_image = comp16[...] * jnp.sum(fr[it].astype(F32), axis=0)
        new_resid = new_image - x
        acc_r = jnp.zeros((HALF, 128), F32)
        acc_d = jnp.zeros((HALF, 128), F32)
        if it == 0:
            for k in range(3 * sub):
                acc_r = acc_r + hist[k] * new_resid[k : k + 1]
        else:
            newest = new_resid - resid
            shift = new_image - image
            for k in range(3 * sub):
                hist[k, order : order + 1] = newest[k : k + 1]
                upd[k, order : order + 1] = shift[k : k + 1]
            for k in range(3 * sub):
                acc_r = acc_r + hist[k] * new_resid[k : k + 1]
                acc_d = acc_d + hist[k] * newest[k : k + 1]
        resid, image = new_resid, new_image
        acc = jnp.concatenate([acc_d, acc_r], axis=0)
        sums = lax.dot_general(jnp.ones((8, 128), F32), acc, NT, precision=HIGH, preferred_element_type=F32)
        bg[it, me] = sums[0:1]
        send_all(bg.at[it, me], b_send.at[it], b_recv.at[it])

        if it == 0:
            @pl.when(me < owners)
            def _():
                wait_bytes(gf.at[pl.ds(0, owners - 1)], g_recv.at[1])

            @pl.when(me >= owners)
            def _():
                wait_bytes(gf, g_recv.at[1])

            gram_all = gf[...].reshape(HALF, 128)
            trace = jnp.sum(jnp.where(lanes == rows, gram_all, 0.0), keepdims=True)
            ridge = ridge_share * trace / order
            inside = (rows < order)
            matrix = gram_all + jnp.where(lanes == rows, jnp.where(inside, ridge, 1.0), 0.0)
            matrix = matrix + jnp.where(lanes == rows + HALF, 1.0, 0.0)
            with jax.named_scope("solve1"):
                inverse = eliminate(matrix[:tall], 0, order)
            for copy in upd_copies:
                copy.wait()

        with jax.named_scope("wait_b"):
            wait_bytes(bg.at[it, pl.ds(0, nd - 1)], b_recv.at[it])
        sums = jnp.sum(bg[it], axis=0)
        if it == 0:
            coef = -jnp.sum(jnp.where(lanes[:tall] >= HALF, inverse * sums, 0.0), axis=1, keepdims=True)
        else:
            column = jnp.sum(jnp.where(lanes == rows, sums, 0.0), axis=1, keepdims=True)
            right = jnp.sum(jnp.where(lanes == rows + HALF, sums, 0.0), axis=1, keepdims=True)
            old = (rows >= 1) & (rows < order) & (lanes >= 1) & (lanes < order)
            matrix = jnp.where(old, gram_all, 0.0)
            matrix = jnp.where((rows == order) & (lanes >= 1) & (lanes <= order), sums, matrix)
            matrix = jnp.where((lanes == order) & (rows >= 1) & (rows < order), column, matrix)
            trace = jnp.sum(jnp.where(lanes == rows, matrix, 0.0), keepdims=True)
            ridge = ridge_share * trace / order
            inside = (rows >= 1) & (rows <= order)
            matrix = matrix + jnp.where(lanes == rows, jnp.where(inside, ridge, 1.0), 0.0)
            matrix = jnp.where(lanes == HALF, jnp.where(inside, right, 0.0), matrix)
            with jax.named_scope("solve2"):
                solved = eliminate(matrix[:tall], 1, order + 1)
            coef = -solved[:, HALF : HALF + 1]
        pieces = []
        for k in range(3 * sub):
            pieces.append(jnp.sum(upd[k, :tall] * coef, axis=0, keepdims=True))
        pieces.append(jnp.zeros((slot - 3 * sub, 128), F32))
        change = jnp.concatenate(pieces, axis=0)
        x = image + change
        xg[it + 1, fi, :used] = x[:used].astype(BF16)
        send_x(it + 1)

    for c in range(3):
        disp[0, c] = image[sub * c : sub * c + sub]
        delta[0, c] = change[sub * c : sub * c + sub]

    pick(iters)
    for g in range(groups):
        u = to_fluid(g)
        for c in range(3):
            u_out[c, 8 * g : 8 * g + 8] = u[8 * c : 8 * c + 8]
    out_copies = [
        pltpu.make_async_copy(u_out.at[c], fluid_out.at[c], out_sems.at[c]) for c in range(3)
    ]
    for copy in out_copies:
        copy.start()

    for phase in range(iters + 1):
        wait_bytes(xg.at[phase, pl.ds(0, nf - 1), pl.ds(0, used)], x_send.at[phase])
    for phase in range(iters):
        wait_bytes(fr.at[phase, pl.ds(0, nf - 1), pl.ds(0, used)], f_send.at[phase])
        wait_bytes(bg.at[phase, pl.ds(0, nd - 1)], b_send.at[phase])
    @pl.when(me >= owners)
    def _():
        wait_bytes(gs, g_send.at[0])

    @pl.when(me < owners)
    def _():
        wait_bytes(gs.at[pl.ds(0, owners - 1)], g_send.at[0])
        wait_bytes(gr.at[pl.ds(0, nd - 1)], g_send.at[1])

    for copy in out_copies:
        copy.wait()


def body(load, stiff, mapping, live, dest, local, comp, start, hist, upd, *, nf, ns):
    blocks = mapping.shape[0]
    sub = comp.shape[1]
    order = hist.shape[0]
    iters = 2
    nd = nf * ns
    slot = -(-3 * sub // 16) * 16
    owners = HALF // 8
    vmem = pl.BlockSpec(memory_space=pltpu.VMEM)
    hbm = pl.BlockSpec(memory_space=pl.ANY)
    dma = pltpu.SemaphoreType.DMA
    disp, delta, fluid = pl.pallas_call(
        functools.partial(kernel, nf, ns, (blocks, sub, order, iters)),
        out_shape=(
            jax.ShapeDtypeStruct((1, 3, sub, 128), F32),
            jax.ShapeDtypeStruct((1, 3, sub, 128), F32),
            jax.ShapeDtypeStruct((3, blocks, 128), F32),
        ),
        in_specs=[hbm] * 10,
        out_specs=(vmem, vmem, vmem),
        scratch_shapes=[
            pltpu.VMEM((1, 1), jnp.int32),
            pltpu.VMEM((1, blocks), jnp.int32),
            pltpu.VMEM((1, blocks), jnp.int32),
            pltpu.VMEM((1, 3, sub, 128), F32),
            pltpu.VMEM((1, 3, sub, 128), F32),
            pltpu.VMEM(mapping.shape, BF16),
            pltpu.VMEM((3, blocks, 128), F32),
            pltpu.VMEM((3, blocks, 128), F32),
            pltpu.VMEM((3 * sub, HALF, 128), F32),
            pltpu.VMEM((3 * sub, HALF, 128), F32),
            pltpu.VMEM((slot, 128), F32),
            pltpu.VMEM((slot, 128), F32),
            pltpu.VMEM((4 * blocks, nf * slot), BF16),
            pltpu.VMEM((nf * slot, 4 * blocks), BF16),
            pltpu.VMEM((4 * blocks, 128), F32),
            pltpu.VMEM((4 * blocks, 128), F32),
            pltpu.VMEM((3, blocks, 128), F32),
            pltpu.VMEM((iters + 1, nf, slot, 128), BF16),
            pltpu.VMEM((iters, nf, slot, 128), FORCE_TYPE),
            pltpu.VMEM((iters, nf, slot, 128), FORCE_TYPE),
            pltpu.VMEM((iters, nd, 1, 128), F32),
            pltpu.VMEM((owners, 8, 128), F32),
            pltpu.VMEM((nd, 8, 128), F32),
            pltpu.VMEM((owners, 8, 128), F32),
            dma((5,)),
            dma((7 + 6 * sub,)),
            dma((3,)),
            dma((iters + 1,)),
            dma((iters + 1,)),
            dma((iters,)),
            dma((iters,)),
            dma((iters,)),
            dma((iters,)),
            dma((2,)),
            dma((2,)),
        ],
        compiler_params=pltpu.CompilerParams(collective_id=0, has_side_effects=True, vmem_limit_bytes=63400000),
    )(
        load.transpose(1, 0, 2), stiff.transpose(1, 0, 2), mapping, live.reshape(1, 1),
        dest.reshape(1, blocks), local.reshape(1, blocks),
        comp.transpose(0, 2, 1, 3), start.transpose(0, 2, 1, 3),
        hist.transpose(0, 1, 3, 2, 4), upd.transpose(0, 1, 3, 2, 4),
    )
    alive = (jnp.arange(blocks) < live[0]).astype(F32)[:, None, None]
    return (disp + delta).transpose(0, 2, 1, 3), fluid.transpose(1, 0, 2) * alive


def solution(mesh):
    in_specs = (
        P(("fluid", "solid"), None, None),
        P(("fluid", "solid"), None, None),
        P(("fluid", "solid"), None, None),
        P(("fluid", "solid")),
        P(("fluid", "solid"), None),
        P(("fluid", "solid")),
        P("solid", "fluid", None, None),
        P("solid", "fluid", None, None),
        P(None, "solid", "fluid", None, None),
        P(None, "solid", "fluid", None, None),
    )
    out_specs = (P("solid", "fluid", None, None), P(("fluid", "solid"), None, None))
    inner = functools.partial(body, nf=mesh.shape["fluid"], ns=mesh.shape["solid"])
    return jax.shard_map(inner, mesh=mesh, in_specs=in_specs, out_specs=out_specs, check_vma=False)
```
